32 devices in a mesh: region: 8 (over z, y), blk: 4 (over x, core).
Axes of the slice: x: 2, y: 2, z: 4, core: 2. Of those that a mesh axis runs over, the one named last changes fastest.
Arguments:
- jac_bus: float32 [256, 8, 128, 128], P('region', 'blk'), may hold values from -0.1875 to 0.1875
- pattern: int32 [256, 8], P(('region', 'blk')), may hold values from 0 to 23
- branch_weight: float32 [256, 128], P(('region', 'blk')), may hold values from 0.2 to 5
- bus_diag: float32 [256, 128], P(('region', 'blk')), may hold values from 0.3 to 3
- right_side: float32 [256, 128], P(('region', 'blk')), may hold values from -8 to 8
Outputs:
- solution: float32 [256, 128], P(('region', 'blk'))
- residual: float32 [256, 128], P(('region', 'blk'))
The draws below stay inside these ranges and needn't reach their ends.
Inputs may be any that keep to these rules, and one draw needn't show every extreme that they name: pattern values below 8 name the region before the branch tile's region, those from 16 the region after it, with regions closed into a loop.
All inputs are finite; a program needn't handle non-finite values.
Results may differ from the reference program's by a relative error of at most 0.0003.
Values sent between devices are 32-bit elements; how exact they have to be, the bound alone decides.
No kernel may reach another device: no remote copies, remote signals or barrier semaphores. Data moves between devices by JAX's collectives and lax.ppermute only.
A program may use at most 64 MiB of HBM per device.

```python
import math
import jax
import jax.numpy as jnp
from jax import lax

TILE = 128
SLOTS_BLK = 2
BR_TILES_DEV = 8
BUS_TILES_DEV = 8
ITERS = 12
SLOTS = 8
TILES = 256
BTILES = 256
N_REGION = 8
N_BLK = 4


def draw_right_side(key, part):
    position = jnp.arange(BTILES, dtype=jnp.float32)[:, None] / BTILES
    scale = 0.6 + 1.2 * position
    values = jax.random.normal(jax.random.fold_in(key, 5), (BTILES, TILE), jnp.float32) * scale
    return jnp.clip(values, -8.0, 8.0)


def set_ends(values, key, low, top_value):
    longest = values.shape.index(max(values.shape))
    spots = []
    for shift in (0, 1):
        where = [jax.random.randint(jax.random.fold_in(key, axis), (), 0, length) for axis, length in enumerate(values.shape)]
        where[longest] = (where[longest] + shift) % values.shape[longest]
        spots.append(tuple(where))
    return values.at[spots[0]].set(low).at[spots[1]].set(top_value)


def shard_levels(rng, shape, shards, low, top_value):
    level, own = 1.0, jax.random.fold_in(rng, 6)
    for dim, shards_of in shards:
        steps = jnp.exp(jax.random.uniform(jax.random.fold_in(own, dim), (shards_of,), jnp.float32, low / len(shards), top_value / len(shards)))
        level = level * jnp.repeat(steps, shape[dim] // shards_of).reshape([-1 if axis == dim else 1 for axis in range(len(shape))])
    return level


def centred(key, extent, deviation, limit, pieces=(), held_as=jnp.bfloat16):
    result = deviation * jax.random.normal(key, extent, jnp.float32)
    if pieces:
        result = result * shard_levels(key, extent, pieces, -0.22, 0.18)
    return jnp.clip(result, -limit, limit).astype(held_as)


def setup_inputs(seed: int = 0) -> dict:
    key_list = jax.random.split(jax.random.key(seed), 6)
    jac_bus = centred(key_list[0], (TILES, SLOTS, TILE, TILE), (TILE * BR_TILES_DEV * N_BLK * SLOTS_BLK // BUS_TILES_DEV) ** -0.5, 0.1875, ((0, 8), (1, 4)), jnp.float32)
    pattern = set_ends(jax.random.randint(key_list[1], (TILES, SLOTS), 0, 3 * BUS_TILES_DEV), jax.random.fold_in(key_list[1], 1), 0, (3 * BUS_TILES_DEV) - 1).astype(jnp.int32)
    branch_weight = jnp.clip(jnp.exp(math.log(5.0) - 3.218876 * jax.random.uniform(key_list[2], (TILES, TILE), jnp.float32) ** shard_levels(key_list[2], (TILES, TILE), ((0, 32),), -0.2, 0.2)), 0.2, 5.0)
    bus_diag = jnp.clip(jnp.exp(math.log(3.0) - 2.3025851 * jax.random.uniform(key_list[3], (BTILES, TILE), jnp.float32) ** shard_levels(key_list[3], (BTILES, TILE), ((0, 32),), -0.2, 0.2)), 0.3, 3.0)
    right_side = draw_right_side(jax.random.fold_in(key_list[5], 71), 0)
    return dict(jac_bus=jac_bus, pattern=pattern, branch_weight=branch_weight, bus_diag=bus_diag, right_side=right_side)


def column_tiles(pattern):
    tiles = jnp.arange(TILES, dtype=jnp.int32)
    region_of = tiles // (N_BLK * BR_TILES_DEV)
    group = jnp.arange(SLOTS, dtype=jnp.int32) // SLOTS_BLK
    offset = pattern // BUS_TILES_DEV
    within = pattern % BUS_TILES_DEV
    owner = (region_of[:, None] + offset - 1) % N_REGION
    return ((owner * N_BLK + group[None, :]) * BUS_TILES_DEV + within).astype(jnp.int32)


def apply_operator(jac_bus, index, branch_weight, bus_diag, vector):
    hp = lax.Precision.HIGHEST
    picked = vector[index]
    rows = jnp.einsum('tjab,tjb->ta', jac_bus, picked, precision=hp)
    weighted = branch_weight * rows
    back = jnp.einsum('tjab,ta->tjb', jac_bus, weighted, precision=hp)
    return bus_diag * vector + jnp.zeros_like(vector).at[index].add(back)


def reference(jac_bus, pattern, branch_weight, bus_diag, right_side):
    hp = lax.Precision.HIGHEST
    index = column_tiles(pattern)
    precond = bus_diag
    for slot in range(SLOTS):
        square = jac_bus[:, slot] * jac_bus[:, slot]
        contrib = jnp.einsum('tab,ta->tb', square, branch_weight, precision=hp)
        precond = precond.at[index[:, slot]].add(contrib)
    solution = jnp.zeros_like(right_side)
    residual = right_side
    scaled = residual / precond
    direction = scaled
    energy = jnp.sum(residual * scaled)
    for step in range(ITERS):
        image = apply_operator(jac_bus, index, branch_weight, bus_diag, direction)
        alpha = energy / jnp.sum(direction * image)
        solution = solution + alpha * direction
        residual = residual - alpha * image
        scaled = residual / precond
        fresh = jnp.sum(residual * scaled)
        direction = scaled + (fresh / energy) * direction
        energy = fresh
    return solution, residual
```

```python
import functools
import jax
import jax.numpy as jnp
from jax import lax
from jax.experimental import pallas as pl
from jax.experimental.pallas import tpu as pltpu
from jax.sharding import PartitionSpec as P

ITERS = 12
SUB = 8
VMEM_LIMIT = 16 * 1024 * 1024
BANKS = 4
UNROLL = 8

vmem = pl.BlockSpec(memory_space=pltpu.VMEM)
smem = pl.BlockSpec(memory_space=pltpu.SMEM)


def rows8(ref_value):
    return ref_value.reshape(-1, SUB, ref_value.shape[-1])


def diagonal(width):
    row = lax.broadcasted_iota(jnp.int32, (width, width), 0)
    lane = lax.broadcasted_iota(jnp.int32, (width, width), 1)
    return rows8(row == lane)


def as_column(row, eye):
    spread = jnp.where(eye, row[None], 0.0)
    return jnp.sum(spread, axis=-1, keepdims=True)


def lane_total(value):
    return jnp.sum(jnp.sum(value, axis=0, keepdims=True), axis=1, keepdims=True)


def forward(jac, index, spread, rows):
    tiles, slots, width, _ = jac.shape
    eye = diagonal(width)

    def tile(t, carry):
        total = None
        for j in range(slots):
            term = rows8(jac[t, j]) * spread[index[t * slots + j]][None]
            total = term if total is None else total + term
        total = jnp.sum(total, axis=-1, keepdims=True)
        rows[pl.ds(t, 1), :] = jnp.sum(
            jnp.sum(jnp.where(eye, total, 0.0), axis=0), axis=0, keepdims=True
        )
        return carry

    lax.fori_loop(0, tiles, tile, 0, unroll=UNROLL)


def backward(jac, index, weighted, banks, square):
    tiles, slots, width, _ = jac.shape
    eye = diagonal(width)
    banks[...] = jnp.zeros_like(banks)

    def tile(t, carry):
        column = as_column(weighted[pl.ds(t, 1), :], eye)
        for j in range(slots):
            block = rows8(jac[t, j])
            if square:
                block = block * block
            where = (lax.rem(t * slots + j, BANKS), index[t * slots + j])
            banks[where] += jnp.sum(block * column, axis=0)
        return carry

    lax.fori_loop(0, tiles, tile, 0, unroll=UNROLL)
    total = banks[0]
    for bank in range(1, BANKS):
        total = total + banks[bank]
    return jnp.sum(total, axis=1)


def publish(chunk, out):
    for member in range(out.shape[0]):
        out[member] = chunk


def diag_kernel(index, jac, weight, diag, rhs, out, banks):
    squares = backward(jac, index, weight, banks, True)
    publish(jnp.concatenate([squares, diag[...], rhs[...]], axis=0), out)


def back_kernel(index, jac, weight, own, *refs):
    others, (out, weighted, banks) = refs[:-3], refs[-3:]
    tiles = jac.shape[0]
    parts = [own] + list(others)
    even, odd = None, None
    for shift, part in enumerate(parts):
        if shift % 2 == 0:
            even = part[...] if even is None else even + part[...]
        else:
            odd = part[...] if odd is None else odd + part[...]
    total = even if odd is None else even + odd
    rows, sums = total[:tiles], total[tiles:]
    weighted[...] = weight[...] * rows
    delta = jnp.sum(weighted[...] * rows, axis=0, keepdims=True) + sums[1:2]
    scalars = jnp.concatenate([sums[:1], delta, sums[2:]], axis=0)
    columns = backward(jac, index, weighted, banks, False)
    publish(jnp.concatenate([columns, scalars], axis=0), out)


def send_rows(jac, index, resid, scaled, diag, spread, own, out):
    tiles = jac.shape[0]
    spread[...] = jnp.broadcast_to(scaled[:, None, :], spread.shape)
    forward(jac, index, spread, out)
    r, z, d = resid[own], scaled[own], diag[own]
    gamma = jnp.sum(r * z, axis=0, keepdims=True)
    delta = jnp.sum(d * z * z, axis=0, keepdims=True)
    pad = jnp.zeros((SUB - 2, z.shape[1]), jnp.float32)
    out[tiles:, :] = jnp.concatenate([gamma, delta, pad], axis=0)


def gathered(received, region, regions, per_dev):
    blocks = []
    for offset in (-1, 0, 1):
        total = None
        for e in (-1, 0, 1):
            source = lax.rem(region + (offset + e + regions), regions)
            start = (1 - e) * per_dev
            term = received[source, start : start + per_dev, :]
            total = term if total is None else total + term
        blocks.append(total)
    return jnp.concatenate(blocks, axis=0)


def halo(received, region, regions, start, per_dev):
    blocks = []
    for offset in (-1, 0, 1):
        source = lax.rem(region + (offset + regions), regions)
        blocks.append(received[source, start : start + per_dev, :])
    return jnp.concatenate(blocks, axis=0)


def first_kernel(place, index, jac, received, out, diag, precond, resid, spread):
    regions = received.shape[0]
    per_dev = diag.shape[0] // 3
    region = place[0]
    extent = 3 * per_dev
    d = halo(received, region, regions, extent, per_dev)
    r = halo(received, region, regions, extent + per_dev, per_dev)
    m = d + gathered(received, region, regions, per_dev)
    diag[...] = d
    precond[...] = m
    resid[...] = r
    own = slice(per_dev, 2 * per_dev)
    send_rows(jac, index, r, r / m, d, spread, own, out)


def update(place, received, diag, precond, resid, along, direct, answer, scal):
    regions = received.shape[0]
    per_dev = direct.shape[0]
    extent = 3 * per_dev
    r, d, m = resid[...], diag[...], precond[...]
    z = r / m
    image = d * z + gathered(received, place[0], regions, per_dev)
    sums = received[0, extent : extent + SUB, :]
    for member in range(1, regions):
        sums = sums + received[member, extent : extent + SUB, :]
    sums = jnp.sum(sums, axis=1, keepdims=True)
    gamma, delta = sums[:1], sums[1:2]
    before, alpha = scal[0:1, :1], scal[1:2, :1]
    started = alpha != 0.0
    beta = jnp.where(started, gamma / jnp.where(started, before, 1.0), 0.0)
    fall = jnp.where(started, beta * gamma / jnp.where(started, alpha, 1.0), 0.0)
    alpha = gamma / (delta - fall)
    s = image + beta * along[...]
    p = z[per_dev : 2 * per_dev] + beta * direct[...]
    x = answer[...] + alpha * p
    return x, r - alpha * s, s, p, gamma, alpha


def step_kernel(
    place, index, jac, received, diag, precond, resid, along, direct, answer, scal,
    out, resid_o, along_o, direct_o, answer_o, scal_o, spread,
):
    per_dev = direct.shape[0]
    x, r, s, p, gamma, alpha = update(
        place, received, diag, precond, resid, along, direct, answer, scal
    )
    resid_o[...] = r
    along_o[...] = s
    direct_o[...] = p
    answer_o[...] = x
    scal_o[0:1, :] = jnp.broadcast_to(gamma, (1, scal_o.shape[1]))
    scal_o[1:2, :] = jnp.broadcast_to(alpha, (1, scal_o.shape[1]))
    own = slice(per_dev, 2 * per_dev)
    send_rows(jac, index, r, r / precond[...], diag, spread, own, out)


def last_kernel(
    place, received, diag, precond, resid, along, direct, answer, scal, answer_o, resid_o
):
    per_dev = direct.shape[0]
    x, r, _, _, _, _ = update(
        place, received, diag, precond, resid, along, direct, answer, scal
    )
    answer_o[...] = x
    resid_o[...] = r[per_dev : 2 * per_dev]


def call(kernel, outs, scratch, specs, name, flops, moved):
    return pl.pallas_call(
        kernel,
        out_shape=[jax.ShapeDtypeStruct(shape, jnp.float32) for shape in outs],
        in_specs=specs,
        out_specs=[vmem] * len(outs),
        scratch_shapes=scratch,
        compiler_params=pltpu.CompilerParams(vmem_limit_bytes=VMEM_LIMIT),
        cost_estimate=pl.CostEstimate(
            flops=flops, bytes_accessed=moved, transcendentals=0
        ),
        name=name,
    )


def body(jac, pattern, branch_weight, bus_diag, right_side):
    blocks = lax.axis_size("blk")
    regions = lax.axis_size("region")
    per_dev, width = right_side.shape
    tiles, slots = jac.shape[:2]
    extent = 3 * per_dev
    f32 = jnp.float32

    def across_blk(value):
        return [
            lax.ppermute(value, "blk", [(i, (i + k) % blocks) for i in range(blocks)])
            for k in range(1, blocks)
        ]

    def across_region(chunks):
        return lax.all_to_all(chunks, "region", 0, 0, tiled=True)

    group = lax.axis_index("blk")
    place = lax.axis_index("region").astype(jnp.int32).reshape(1)
    fits = jnp.pad(pattern.astype(f32), ((0, 0), (0, width - pattern.shape[1])))
    mine = jnp.concatenate([branch_weight, fits], axis=0)
    shared = jnp.stack([mine] + across_blk(mine))
    order = lax.rem(group - jnp.arange(blocks, dtype=jnp.int32) + blocks, blocks)
    shared = shared[order]
    weight = shared[:, : branch_weight.shape[0]].reshape(tiles, width)
    chosen = shared[:, branch_weight.shape[0] :].reshape(tiles, width)
    index = lax.dynamic_slice_in_dim(chosen, group * slots, slots, axis=1)
    index = index.astype(jnp.int32).reshape(-1)

    flops = 4 * jac.size
    moved = 4 * jac.size
    row_count = tiles + SUB
    spread = pltpu.VMEM((extent, SUB, width), f32)
    banks = pltpu.VMEM((BANKS, extent, SUB, width), f32)
    chunk = (regions, extent + SUB, width)
    halo_shape, own_shape = (extent, width), (per_dev, width)

    (setup,) = call(
        diag_kernel, [(regions, extent + 2 * per_dev, width)], [banks],
        [smem, vmem, vmem, vmem, vmem], "diagonal", flops, moved,
    )(index, jac, weight, bus_diag, right_side)
    out, diag, precond, resid = call(
        first_kernel, [(row_count, width), halo_shape, halo_shape, halo_shape],
        [spread], [smem, smem, vmem, vmem], "first", flops, moved,
    )(place, index, jac, across_region(setup))

    def image_of(out):
        parts = across_blk(out)
        (chunks,) = call(
            back_kernel, [chunk], [pltpu.VMEM((tiles, width), f32), banks],
            [smem] + [vmem] * (3 + len(parts)), "back", flops, moved,
        )(index, jac, weight, out, *parts)
        return across_region(chunks)

    def step(i, carry):
        received, resid, along, direct, answer, scal = carry
        out, resid, along, direct, answer, scal = call(
            step_kernel,
            [(row_count, width), halo_shape, halo_shape, own_shape, own_shape, (SUB, width)],
            [spread], [smem, smem] + [vmem] * 9, "step", flops, moved,
        )(place, index, jac, received, diag, precond, resid, along, direct, answer, scal)
        return image_of(out), resid, along, direct, answer, scal

    carry = (
        image_of(out), resid, jnp.zeros(halo_shape, f32), jnp.zeros(own_shape, f32),
        jnp.zeros(own_shape, f32), jnp.zeros((SUB, width), f32),
    )
    carry = lax.fori_loop(0, ITERS - 1, step, carry)
    received, resid, along, direct, answer, scal = carry
    answer, resid = call(
        last_kernel, [own_shape, own_shape], [], [smem] + [vmem] * 8, "last", 1000, 1000
    )(place, received, diag, precond, resid, along, direct, answer, scal)
    return answer, resid


def solution(mesh):
    both = P(("region", "blk"), None)
    return jax.shard_map(
        body,
        mesh=mesh,
        in_specs=(P("region", "blk", None, None), both, both, both, both),
        out_specs=(both, both),
        check_vma=False,
    )
```

```python
import functools
import jax
import jax.numpy as jnp
from jax import lax
from jax.experimental import pallas as pl
from jax.experimental.pallas import tpu as pltpu
from jax.sharding import PartitionSpec as P

ITERS = 12
SUB = 8
SPOTS = {(2, 1): 0, (1, 0): 0, (1, 1): 1, (-1, -1): 0, (-1, 0): 1, (-2, -1): 1}
VMEM_LIMIT = 16 * 1024 * 1024
BANKS = 4
PIECES = 8

vmem = pl.BlockSpec(memory_space=pltpu.VMEM)
anywhere = pl.BlockSpec(memory_space=pl.ANY)
hbm = pl.BlockSpec(memory_space=pltpu.HBM)


def rows8(ref_value):
    return ref_value.reshape(-1, SUB, ref_value.shape[-1])


def diagonal(width):
    row = lax.broadcasted_iota(jnp.int32, (width, width), 0)
    lane = lax.broadcasted_iota(jnp.int32, (width, width), 1)
    return rows8(row == lane)


def as_column(row, eye):
    spread = jnp.where(eye, row[None], 0.0)
    return jnp.sum(spread, axis=-1, keepdims=True)


def lane_total(value):
    return jnp.sum(jnp.sum(value, axis=0, keepdims=True), axis=1, keepdims=True)


def copy_in(source, target, sem):
    return pltpu.make_async_copy(source, target, sem)


def forward(jac, index, spread, rows):
    tiles, slots, width, _ = jac.shape
    eye = diagonal(width)
    for t in range(tiles):
        total = None
        for j in range(slots):
            term = rows8(jac[t, j]) * spread[index[t * slots + j]][None]
            total = term if total is None else total + term
        total = jnp.sum(total, axis=-1, keepdims=True)
        rows[t : t + 1, :] = jnp.sum(
            jnp.sum(jnp.where(eye, total, 0.0), axis=0), axis=0, keepdims=True
        )


def backward(jac, chosen, weighted, banks, back, ready, square, arrived=lambda t: None):
    tiles, slots, width, _ = jac.shape
    eye = diagonal(width)
    banks[...] = jnp.zeros_like(banks)

    def add(t):
        for j in range(slots):
            where = ((t * slots + j) % BANKS, chosen(t, j))
            banks[where] += back[t * slots + j]

    half = tiles // 2
    for t in range(tiles):
        arrived(t)
        if t == half:
            ready()
            for early in range(half):
                add(early)
        column = as_column(weighted[t : t + 1, :], eye)
        for j in range(slots):
            block = rows8(jac[t, j])
            if square:
                block = block * block
            back[t * slots + j] = jnp.sum(block * column, axis=0)
        if t >= half:
            add(t)
    total = banks[0]
    for bank in range(1, BANKS):
        total = total + banks[bank]
    return jnp.sum(total, axis=1)


def publish(chunk, out):
    for member in range(out.shape[0]):
        out[member] = chunk


def place_blocks(out, keep, columns, scalars):
    regions, per_dev = out.shape[0], columns.shape[0] // 3
    region = lax.axis_index("region")
    first, middle, last = (
        columns[n * per_dev : (n + 1) * per_dev] for n in range(3)
    )
    keep[...] = jnp.concatenate([columns, scalars], axis=0)
    blank = jnp.concatenate([jnp.zeros_like(first)] * 2 + [scalars], axis=0)
    for away in range(3, regions - 2):
        out[lax.rem(region + away, regions)] = blank
    zero = jnp.zeros_like(first)
    for away, pair in (
        (-2, (first, zero)), (-1, (first, middle)), (1, (middle, last)), (2, (zero, last)),
    ):
        target = lax.rem(region + (away + regions), regions)
        out[target] = jnp.concatenate([*pair, scalars], axis=0)
    out[region] = blank


def diag_kernel(jac, vectors, *refs):
    ins, refs = refs[:-10], refs[-10:]
    out, weight, place, held, fits, index, small, banks, back, sems = refs
    tiles, slots = jac.shape[:2]
    blocks = len(ins)
    per_dev = tiles // blocks
    step = tiles // PIECES
    pieces = [
        copy_in(
            jac.at[pl.ds(n * step, step)], held.at[pl.ds(n * step, step)], sems.at[n]
        )
        for n in range(PIECES)
    ]
    for copy in pieces:
        copy.start()
    group = lax.axis_index("blk")
    for shift, part in enumerate(ins):
        source = lax.rem(group + (blocks - shift), blocks)
        spot = pl.ds(pl.multiple_of(source * per_dev, per_dev), per_dev)
        weight[spot, :] = part[:per_dev, :]
        fits[spot, :] = part[per_dev:, :].astype(jnp.int32)
    table = copy_in(fits, index, sems.at[PIECES])
    table.start()
    listed = copy_in(small, place, sems.at[PIECES + 1])

    def ready():
        table.wait()
        for t in range(tiles):
            for j in range(slots):
                small[t * slots + j] = index[t, group * slots + j]
        listed.start()

    def arrived(t):
        if t % step == 0:
            pieces[t // step].wait()

    squares = backward(
        held, lambda t, j: small[t * slots + j], weight, banks, back, ready, True, arrived
    )
    publish(jnp.concatenate([squares, vectors[...]], axis=0), out)
    listed.wait()


def back_kernel(place, jac, weight, own, *refs):
    others, refs = refs[:-7], refs[-7:]
    out, keep, weighted, banks, back, index, sem = refs
    copy = copy_in(place, index, sem)
    copy.start()
    tiles, slots = jac.shape[:2]
    parts = [own] + list(others)
    even, odd = None, None
    for shift, part in enumerate(parts):
        if shift % 2 == 0:
            even = part[...] if even is None else even + part[...]
        else:
            odd = part[...] if odd is None else odd + part[...]
    total = even if odd is None else even + odd
    rows, sums = total[:tiles], total[tiles:]
    weighted[...] = weight[...] * rows
    delta = jnp.sum(weighted[...] * rows, axis=0, keepdims=True) + sums[1:2]
    scalars = jnp.concatenate([sums[:1], delta, sums[2:]], axis=0)
    columns = backward(
        jac, lambda t, j: index[t * slots + j], weighted, banks, back, copy.wait, False
    )
    place_blocks(out, keep, columns, scalars)


def send_rows(jac, index, resid, scaled, diag, spread, own, out):
    tiles = jac.shape[0]
    spread[...] = jnp.broadcast_to(scaled[:, None, :], spread.shape)
    forward(jac, index, spread, out)
    r, z, d = resid[own], scaled[own], diag[own]
    gamma = jnp.sum(r * z, axis=0, keepdims=True)
    delta = jnp.sum(d * z * z, axis=0, keepdims=True)
    pad = jnp.zeros((SUB - 2, z.shape[1]), jnp.float32)
    out[tiles:, :] = jnp.concatenate([gamma, delta, pad], axis=0)


def gathered(received, region, regions, per_dev):
    blocks = []
    for offset in (-1, 0, 1):
        total = None
        for e in (-1, 0, 1):
            source = lax.rem(region + (offset + e + regions), regions)
            start = (1 - e) * per_dev
            term = received[source, start : start + per_dev, :]
            total = term if total is None else total + term
        blocks.append(total)
    return jnp.concatenate(blocks, axis=0)


def halo(received, region, regions, start, per_dev):
    blocks = []
    for offset in (-1, 0, 1):
        source = lax.rem(region + (offset + regions), regions)
        blocks.append(received[source, start : start + per_dev, :])
    return jnp.concatenate(blocks, axis=0)


def first_kernel(
    place, jac, received, out, diag, precond, resid, spread, index, sem
):
    copy = copy_in(place, index, sem)
    copy.start()
    regions = received.shape[0]
    per_dev = diag.shape[0] // 3
    region = lax.axis_index("region")
    extent = 3 * per_dev
    d = halo(received, region, regions, extent, per_dev)
    r = halo(received, region, regions, extent + per_dev, per_dev)
    m = d + gathered(received, region, regions, per_dev)
    diag[...] = d
    precond[...] = m
    resid[...] = r
    own = slice(per_dev, 2 * per_dev)
    copy.wait()
    send_rows(jac, index, r, r / m, d, spread, own, out)


def collected(received, kept, per_dev):
    regions = received.shape[0]
    region = lax.axis_index("region")
    blocks = []
    for offset in (-1, 0, 1):
        total = None
        for e in (-1, 0, 1):
            away = offset + e
            if away == 0:
                start = (1 - e) * per_dev
                term = kept[start : start + per_dev, :]
            else:
                source = lax.rem(region + (away + regions), regions)
                start = SPOTS[away, offset] * per_dev
                term = received[source, start : start + per_dev, :]
            total = term if total is None else total + term
        blocks.append(total)
    return jnp.concatenate(blocks, axis=0)


def update(received, kept, diag, precond, resid, along, direct, answer, scal):
    regions = received.shape[0]
    per_dev = direct.shape[0]
    r, d, m = resid[...], diag[...], precond[...]
    z = r / m
    image = d * z + collected(received, kept, per_dev)
    region = lax.axis_index("region")
    sums = None
    for member in range(regions):
        term = jnp.where(
            region == member, kept[3 * per_dev :, :], received[member, 2 * per_dev :, :]
        )
        sums = term if sums is None else sums + term
    sums = jnp.sum(sums, axis=1, keepdims=True)
    gamma, delta = sums[:1], sums[1:2]
    before, alpha = scal[0:1, :1], scal[1:2, :1]
    started = alpha != 0.0
    beta = jnp.where(started, gamma / jnp.where(started, before, 1.0), 0.0)
    fall = jnp.where(started, beta * gamma / jnp.where(started, alpha, 1.0), 0.0)
    alpha = gamma / (delta - fall)
    s = image + beta * along[...]
    p = z[per_dev : 2 * per_dev] + beta * direct[...]
    x = answer[...] + alpha * p
    return x, r - alpha * s, s, p, gamma, alpha


def step_kernel(
    place, jac, received, kept, diag, precond, resid, along, direct, answer, scal,
    out, resid_o, along_o, direct_o, answer_o, scal_o, spread, index, sem,
):
    copy = copy_in(place, index, sem)
    copy.start()
    per_dev = direct.shape[0]
    x, r, s, p, gamma, alpha = update(
        received, kept, diag, precond, resid, along, direct, answer, scal
    )
    resid_o[...] = r
    along_o[...] = s
    direct_o[...] = p
    answer_o[...] = x
    scal_o[0:1, :] = jnp.broadcast_to(gamma, (1, scal_o.shape[1]))
    scal_o[1:2, :] = jnp.broadcast_to(alpha, (1, scal_o.shape[1]))
    own = slice(per_dev, 2 * per_dev)
    copy.wait()
    send_rows(jac, index, r, r / precond[...], diag, spread, own, out)


def last_kernel(
    received, kept, diag, precond, resid, along, direct, answer, scal, answer_o,
    resid_o,
):
    per_dev = direct.shape[0]
    x, r, _, _, _, _ = update(
        received, kept, diag, precond, resid, along, direct, answer, scal
    )
    answer_o[...] = x
    resid_o[...] = r[per_dev : 2 * per_dev]


def call(kernel, outs, scratch, specs, name, flops, moved, limit=VMEM_LIMIT):
    outs = [
        shape
        if isinstance(shape, jax.ShapeDtypeStruct)
        else jax.ShapeDtypeStruct(shape, jnp.float32)
        for shape in outs
    ]
    return pl.pallas_call(
        kernel,
        out_shape=outs,
        in_specs=specs,
        out_specs=[vmem] * len(outs),
        scratch_shapes=scratch,
        compiler_params=pltpu.CompilerParams(vmem_limit_bytes=limit),
        cost_estimate=pl.CostEstimate(
            flops=flops, bytes_accessed=moved, transcendentals=0
        ),
        name=name,
    )


def body(jac, pattern, branch_weight, bus_diag, right_side):
    blocks = lax.axis_size("blk")
    regions = lax.axis_size("region")
    per_dev, width = right_side.shape
    tiles, slots = jac.shape[:2]
    extent = 3 * per_dev
    f32 = jnp.float32

    def across_blk(value):
        return [
            lax.ppermute(value, "blk", [(i, (i + k) % blocks) for i in range(blocks)])
            for k in range(1, blocks)
        ]

    def across_region(chunks):
        return lax.all_to_all(chunks, "region", 0, 0, tiled=True)

    flops = 4 * jac.size
    moved = 4 * jac.size
    row_count = tiles + SUB
    spread = pltpu.VMEM((extent, SUB, width), f32)
    banks = pltpu.VMEM((BANKS, extent, SUB, width), f32)
    back = pltpu.VMEM((tiles * slots, SUB, width), f32)
    table = [pltpu.SMEM((tiles * slots,), jnp.int32), pltpu.SemaphoreType.DMA]
    chunk = (regions, 2 * per_dev + SUB, width)
    kept_shape = (extent + SUB, width)
    halo_shape, own_shape = (extent, width), (per_dev, width)

    fits = jnp.pad(pattern, ((0, 0), (0, width - pattern.shape[1]))).astype(f32)
    vectors = jnp.concatenate([bus_diag, right_side], axis=0)
    mine = jnp.concatenate([branch_weight, fits], axis=0)
    setup, weight, place, jac = call(
        diag_kernel,
        [
            (regions, extent + 2 * per_dev, width), (tiles, width),
            jax.ShapeDtypeStruct((tiles * slots,), jnp.int32), jac.shape,
        ],
        [
            pltpu.VMEM((tiles, width), jnp.int32), pltpu.SMEM((tiles, width), jnp.int32),
            pltpu.SMEM((tiles * slots,), jnp.int32), banks, back,
            pltpu.SemaphoreType.DMA((PIECES + 2,)),
        ],
        [hbm] + [vmem] * (1 + blocks), "diagonal", flops, moved, 47 * 1024 * 1024,
    )(jac, vectors, mine, *across_blk(mine))
    setup = across_region(setup)
    out, diag, precond, resid = call(
        first_kernel, [(row_count, width), halo_shape, halo_shape, halo_shape],
        [spread] + table, [anywhere, vmem, vmem],
        "first", flops, moved,
    )(place, jac, setup)

    def image_of(out):
        parts = across_blk(out)
        chunks, kept = call(
            back_kernel, [chunk, kept_shape], [pltpu.VMEM((tiles, width), f32), banks, back] + table,
            [anywhere] + [vmem] * (3 + len(parts)),
            "back", flops, moved,
        )(place, jac, weight, out, *parts)
        return across_region(chunks), kept

    def step(carry):
        received, kept, resid, along, direct, answer, scal = carry
        out, resid, along, direct, answer, scal = call(
            step_kernel,
            [(row_count, width), halo_shape, halo_shape, own_shape, own_shape, (SUB, width)],
            [spread] + table, [anywhere] + [vmem] * 10,
            "step", flops, moved,
        )(place, jac, received, kept, diag, precond, resid, along, direct, answer, scal)
        return *image_of(out), resid, along, direct, answer, scal

    carry = (
        *image_of(out), resid, jnp.zeros(halo_shape, f32), jnp.zeros(own_shape, f32),
        jnp.zeros(own_shape, f32), jnp.zeros((SUB, width), f32),
    )
    for _ in range(ITERS - 1):
        carry = step(carry)
    received, kept, resid, along, direct, answer, scal = carry
    answer, resid = call(
        last_kernel, [own_shape, own_shape], [], [vmem] * 9, "last", 1000, 1000
    )(received, kept, diag, precond, resid, along, direct, answer, scal)
    return answer, resid


def solution(mesh):
    both = P(("region", "blk"), None)
    return jax.shard_map(
        body,
        mesh=mesh,
        in_specs=(P("region", "blk", None, None), both, both, both, both),
        out_specs=(both, both),
        check_vma=False,
    )
```

```python
import functools
import jax
import jax.numpy as jnp
from jax import lax
from jax.experimental import pallas as pl
from jax.experimental.pallas import tpu as pltpu
from jax.sharding import PartitionSpec as P

ITERS = 12
SUB = 8
SPOTS = {(2, 1): 0, (1, 0): 0, (1, 1): 1, (-1, -1): 0, (-1, 0): 1, (-2, -1): 1}
VMEM_LIMIT = 16 * 1024 * 1024
PIECES = 8

vmem = pl.BlockSpec(memory_space=pltpu.VMEM)
hbm = pl.BlockSpec(memory_space=pltpu.HBM)


def rows8(ref_value):
    return ref_value.reshape(-1, SUB, ref_value.shape[-1])


def diagonal(width):
    row = lax.broadcasted_iota(jnp.int32, (width, width), 0)
    lane = lax.broadcasted_iota(jnp.int32, (width, width), 1)
    return rows8(row == lane)


def three_terms(value):
    high = value.astype(jnp.bfloat16).astype(jnp.float32)
    middle = (value - high).astype(jnp.bfloat16).astype(jnp.float32)
    return high, middle, (value - high) - middle


def selectors(tiles, width):
    shape = (tiles // 2, width, 2 * width)
    pair, row, lane = (lax.broadcasted_iota(jnp.int32, shape, n) for n in range(3))
    wanted = 2 * pair + lane // width
    return ((row % tiles == wanted) & (row < 3 * tiles)).astype(jnp.bfloat16)


def copy_in(source, target, sem):
    return pltpu.make_async_copy(source, target, sem)


def gather_rows(scaled, lookup, picked):
    slots, tiles, width = lookup.shape
    groups = [scaled[n : n + SUB] for n in range(0, scaled.shape[0], SUB)]
    for j in range(slots):
        for start in range(0, tiles, SUB):
            wanted = lookup[j, start : start + SUB, :]
            within = lax.rem(wanted, SUB)
            total = None
            for n, group in enumerate(groups):
                found = jnp.take_along_axis(
                    group, within, axis=0, mode="promise_in_bounds"
                )
                found = jnp.where(wanted // SUB == n, found, 0.0)
                total = found if total is None else total + found
            picked[j, start : start + SUB, :] = total


def forward(jac, picked, rows):
    tiles, slots, width, _ = jac.shape
    eye = diagonal(width)
    for t in range(tiles):
        total = None
        for j in range(slots):
            term = rows8(jac[t, j]) * picked[j, t : t + 1, :][None]
            total = term if total is None else total + term
        total = jnp.sum(total, axis=-1, keepdims=True)
        rows[t : t + 1, :] = jnp.sum(
            jnp.sum(jnp.where(eye, total, 0.0), axis=0), axis=0, keepdims=True
        )


def backward(jac, weighted, picks, spots, back, square, arrived=lambda t: None):
    tiles, slots, width, _ = jac.shape
    value = weighted[...]
    terms = three_terms(value)
    rest = jnp.zeros((width - 3 * tiles, width), jnp.float32)
    turned = jnp.transpose(jnp.concatenate([*terms, rest], axis=0))
    turned = turned.astype(jnp.bfloat16)
    for t in range(tiles):
        arrived(t)
        if t % 2 == 0:
            both = jnp.dot(turned, picks[t // 2], preferred_element_type=jnp.float32)
        column = rows8(both[:, t % 2 * width : (t % 2 + 1) * width])
        for j in range(slots):
            block = rows8(jac[t, j])
            if square:
                block = block * block
            back[j * tiles + t : j * tiles + t + 1, :] = jnp.sum(
                jnp.sum(block * column, axis=0), axis=0, keepdims=True
            )
    terms = three_terms(back[...])
    stacked = jnp.concatenate([*terms, jnp.zeros_like(terms[0])], axis=0)
    return jnp.dot(
        spots[...], stacked.astype(jnp.bfloat16), preferred_element_type=jnp.float32
    )


def publish(chunk, out):
    for member in range(out.shape[0]):
        out[member] = chunk


def place_blocks(out, keep, columns, scalars):
    regions, per_dev = out.shape[0], columns.shape[0] // 3
    region = lax.axis_index("region")
    first, middle, last = (
        columns[n * per_dev : (n + 1) * per_dev] for n in range(3)
    )
    keep[...] = jnp.concatenate([columns, scalars], axis=0)
    blank = jnp.concatenate([jnp.zeros_like(first)] * 2 + [scalars], axis=0)
    for away in range(3, regions - 2):
        out[lax.rem(region + away, regions)] = blank
    zero = jnp.zeros_like(first)
    for away, pair in (
        (-2, (first, zero)), (-1, (first, middle)), (1, (middle, last)), (2, (zero, last)),
    ):
        target = lax.rem(region + (away + regions), regions)
        out[target] = jnp.concatenate([*pair, scalars], axis=0)
    out[region] = blank


def diag_kernel(jac, vectors, picks, *refs):
    ins, refs = refs[:-8], refs[-8:]
    out, weight, spots, held, lookup, fits, back, sems = refs
    tiles, slots, width, _ = jac.shape
    blocks = len(ins)
    per_dev = tiles // blocks
    step = tiles // PIECES
    pieces = [
        copy_in(
            jac.at[pl.ds(n * step, step)], held.at[pl.ds(n * step, step)], sems.at[n]
        )
        for n in range(PIECES)
    ]
    for copy in pieces:
        copy.start()
    group = lax.axis_index("blk")
    for shift, part in enumerate(ins):
        source = lax.rem(group + (blocks - shift), blocks)
        spot = pl.ds(pl.multiple_of(source * per_dev, per_dev), per_dev)
        weight[spot, :] = part[:per_dev, :]
        fits[spot, :] = part[per_dev:, :]
    lane = lax.broadcasted_iota(jnp.int32, fits.shape, 1)
    chosen = []
    for j in range(slots):
        own = jnp.where(lane == group * slots + j, fits[...], 0.0)
        own = jnp.sum(own, axis=1, keepdims=True)
        chosen.append(jnp.broadcast_to(own, fits.shape))
        lookup[j] = chosen[j].astype(jnp.int32)
    unused = jnp.full((slots * tiles, width), -1.0, jnp.float32)
    names = jnp.transpose(jnp.concatenate(chosen * 3 + [unused], axis=0))
    names = names[: spots.shape[0]].astype(jnp.int32)
    column = lax.broadcasted_iota(jnp.int32, names.shape, 0)
    spots[...] = jnp.where(column == names, 1.0, 0.0).astype(jnp.bfloat16)

    def arrived(t):
        if t % step == 0:
            pieces[t // step].wait()

    squares = backward(held, weight, picks, spots, back, True, arrived)
    publish(jnp.concatenate([squares, vectors[...]], axis=0), out)


def back_kernel(jac, weight, picks, spots, own, *refs):
    others, (out, keep, weighted, back) = refs[:-4], refs[-4:]
    tiles, slots = jac.shape[:2]
    parts = [own] + list(others)
    even, odd = None, None
    for shift, part in enumerate(parts):
        if shift % 2 == 0:
            even = part[...] if even is None else even + part[...]
        else:
            odd = part[...] if odd is None else odd + part[...]
    total = even if odd is None else even + odd
    rows, sums = total[:tiles], total[tiles:]
    weighted[...] = weight[...] * rows
    delta = jnp.sum(weighted[...] * rows, axis=0, keepdims=True) + sums[1:2]
    scalars = jnp.concatenate([sums[:1], delta, sums[2:]], axis=0)
    columns = backward(jac, weighted, picks, spots, back, False)
    place_blocks(out, keep, columns, scalars)


def send_rows(jac, lookup, resid, scaled, diag, picked, own, out):
    tiles = jac.shape[0]
    gather_rows(scaled, lookup, picked)
    forward(jac, picked, out)
    r, z, d = resid[own], scaled[own], diag[own]
    gamma = jnp.sum(r * z, axis=0, keepdims=True)
    delta = jnp.sum(d * z * z, axis=0, keepdims=True)
    pad = jnp.zeros((SUB - 2, z.shape[1]), jnp.float32)
    out[tiles:, :] = jnp.concatenate([gamma, delta, pad], axis=0)


def gathered(received, region, regions, per_dev):
    blocks = []
    for offset in (-1, 0, 1):
        total = None
        for e in (-1, 0, 1):
            source = lax.rem(region + (offset + e + regions), regions)
            start = (1 - e) * per_dev
            term = received[source, start : start + per_dev, :]
            total = term if total is None else total + term
        blocks.append(total)
    return jnp.concatenate(blocks, axis=0)


def halo(received, region, regions, start, per_dev):
    blocks = []
    for offset in (-1, 0, 1):
        source = lax.rem(region + (offset + regions), regions)
        blocks.append(received[source, start : start + per_dev, :])
    return jnp.concatenate(blocks, axis=0)


def first_kernel(jac, lookup, received, out, diag, precond, resid, picked):
    regions = received.shape[0]
    per_dev = diag.shape[0] // 3
    region = lax.axis_index("region")
    extent = 3 * per_dev
    d = halo(received, region, regions, extent, per_dev)
    r = halo(received, region, regions, extent + per_dev, per_dev)
    m = d + gathered(received, region, regions, per_dev)
    diag[...] = d
    precond[...] = m
    resid[...] = r
    own = slice(per_dev, 2 * per_dev)
    send_rows(jac, lookup, r, r / m, d, picked, own, out)


def collected(received, kept, per_dev):
    regions = received.shape[0]
    region = lax.axis_index("region")
    blocks = []
    for offset in (-1, 0, 1):
        total = None
        for e in (-1, 0, 1):
            away = offset + e
            if away == 0:
                start = (1 - e) * per_dev
                term = kept[start : start + per_dev, :]
            else:
                source = lax.rem(region + (away + regions), regions)
                start = SPOTS[away, offset] * per_dev
                term = received[source, start : start + per_dev, :]
            total = term if total is None else total + term
        blocks.append(total)
    return jnp.concatenate(blocks, axis=0)


def update(received, kept, diag, precond, resid, along, direct, answer, scal):
    regions = received.shape[0]
    per_dev = direct.shape[0]
    r, d, m = resid[...], diag[...], precond[...]
    z = r / m
    image = d * z + collected(received, kept, per_dev)
    region = lax.axis_index("region")
    sums = None
    for member in range(regions):
        term = jnp.where(
            region == member, kept[3 * per_dev :, :], received[member, 2 * per_dev :, :]
        )
        sums = term if sums is None else sums + term
    sums = jnp.sum(sums, axis=1, keepdims=True)
    gamma, delta = sums[:1], sums[1:2]
    before, alpha = scal[0:1, :1], scal[1:2, :1]
    started = alpha != 0.0
    beta = jnp.where(started, gamma / jnp.where(started, before, 1.0), 0.0)
    fall = jnp.where(started, beta * gamma / jnp.where(started, alpha, 1.0), 0.0)
    alpha = gamma / (delta - fall)
    s = image + beta * along[...]
    p = z[per_dev : 2 * per_dev] + beta * direct[...]
    x = answer[...] + alpha * p
    return x, r - alpha * s, s, p, gamma, alpha


def step_kernel(
    jac, lookup, received, kept, diag, precond, resid, along, direct, answer, scal,
    out, resid_o, along_o, direct_o, answer_o, scal_o, picked,
):
    per_dev = direct.shape[0]
    x, r, s, p, gamma, alpha = update(
        received, kept, diag, precond, resid, along, direct, answer, scal
    )
    resid_o[...] = r
    along_o[...] = s
    direct_o[...] = p
    answer_o[...] = x
    scal_o[0:1, :] = jnp.broadcast_to(gamma, (1, scal_o.shape[1]))
    scal_o[1:2, :] = jnp.broadcast_to(alpha, (1, scal_o.shape[1]))
    own = slice(per_dev, 2 * per_dev)
    send_rows(jac, lookup, r, r / precond[...], diag, picked, own, out)


def last_kernel(
    received, kept, diag, precond, resid, along, direct, answer, scal, answer_o,
    resid_o,
):
    per_dev = direct.shape[0]
    x, r, _, _, _, _ = update(
        received, kept, diag, precond, resid, along, direct, answer, scal
    )
    answer_o[...] = x
    resid_o[...] = r[per_dev : 2 * per_dev]


def call(kernel, outs, scratch, specs, name, flops, moved, limit=VMEM_LIMIT):
    outs = [
        shape
        if isinstance(shape, jax.ShapeDtypeStruct)
        else jax.ShapeDtypeStruct(shape, jnp.float32)
        for shape in outs
    ]
    return pl.pallas_call(
        kernel,
        out_shape=outs,
        in_specs=specs,
        out_specs=[vmem] * len(outs),
        scratch_shapes=scratch,
        compiler_params=pltpu.CompilerParams(vmem_limit_bytes=limit),
        cost_estimate=pl.CostEstimate(
            flops=flops, bytes_accessed=moved, transcendentals=0
        ),
        name=name,
    )


def body(jac, pattern, branch_weight, bus_diag, right_side):
    blocks = lax.axis_size("blk")
    regions = lax.axis_size("region")
    per_dev, width = right_side.shape
    tiles, slots = jac.shape[:2]
    extent = 3 * per_dev
    f32 = jnp.float32

    def across_blk(value):
        return [
            lax.ppermute(value, "blk", [(i, (i + k) % blocks) for i in range(blocks)])
            for k in range(1, blocks)
        ]

    def across_region(chunks):
        return lax.all_to_all(chunks, "region", 0, 0, tiled=True)

    flops = 4 * jac.size
    moved = 4 * jac.size
    row_count = tiles + SUB
    picked = pltpu.VMEM((slots, tiles, width), f32)
    back = pltpu.VMEM((tiles * slots, width), f32)
    chunk = (regions, 2 * per_dev + SUB, width)
    kept_shape = (extent + SUB, width)
    halo_shape, own_shape = (extent, width), (per_dev, width)

    fits = jnp.pad(pattern, ((0, 0), (0, width - pattern.shape[1]))).astype(f32)
    vectors = jnp.concatenate([bus_diag, right_side], axis=0)
    mine = jnp.concatenate([branch_weight, fits], axis=0)
    picks = selectors(tiles, width)
    setup, weight, spots, jac, lookup = call(
        diag_kernel,
        [
            (regions, extent + 2 * per_dev, width), (tiles, width),
            jax.ShapeDtypeStruct((extent, 4 * tiles * slots), jnp.bfloat16), jac.shape,
            jax.ShapeDtypeStruct((slots, tiles, width), jnp.int32),
        ],
        [
            pltpu.VMEM((tiles, width), f32), back, pltpu.SemaphoreType.DMA((PIECES,)),
        ],
        [hbm] + [vmem] * (2 + blocks), "diagonal", flops, moved, 47 * 1024 * 1024,
    )(jac, vectors, picks, mine, *across_blk(mine))
    setup = across_region(setup)
    out, diag, precond, resid = call(
        first_kernel, [(row_count, width), halo_shape, halo_shape, halo_shape],
        [picked], [vmem] * 3, "first", flops, moved,
    )(jac, lookup, setup)

    def image_of(out):
        parts = across_blk(out)
        chunks, kept = call(
            back_kernel, [chunk, kept_shape], [pltpu.VMEM((tiles, width), f32), back],
            [vmem] * (5 + len(parts)), "back", flops, moved,
        )(jac, weight, picks, spots, out, *parts)
        return across_region(chunks), kept

    def step(carry):
        received, kept, resid, along, direct, answer, scal = carry
        out, resid, along, direct, answer, scal = call(
            step_kernel,
            [(row_count, width), halo_shape, halo_shape, own_shape, own_shape, (SUB, width)],
            [picked], [vmem] * 11, "step", flops, moved,
        )(jac, lookup, received, kept, diag, precond, resid, along, direct, answer, scal)
        return *image_of(out), resid, along, direct, answer, scal

    carry = (
        *image_of(out), resid, jnp.zeros(halo_shape, f32), jnp.zeros(own_shape, f32),
        jnp.zeros(own_shape, f32), jnp.zeros((SUB, width), f32),
    )
    for _ in range(ITERS - 1):
        carry = step(carry)
    received, kept, resid, along, direct, answer, scal = carry
    answer, resid = call(
        last_kernel, [own_shape, own_shape], [], [vmem] * 9, "last", 1000, 1000
    )(received, kept, diag, precond, resid, along, direct, answer, scal)
    return answer, resid


def solution(mesh):
    both = P(("region", "blk"), None)
    return jax.shard_map(
        body,
        mesh=mesh,
        in_specs=(P("region", "blk", None, None), both, both, both, both),
        out_specs=(both, both),
        check_vma=False,
    )
```

```python
import functools
import jax
import jax.numpy as jnp
from jax import lax
from jax.experimental import pallas as pl
from jax.experimental.pallas import tpu as pltpu
from jax.sharding import PartitionSpec as P

ITERS = 12
SUB = 8
SPOTS = {(2, 1): 0, (1, 0): 0, (1, 1): 1, (-1, -1): 0, (-1, 0): 1, (-2, -1): 1}
VMEM_LIMIT = 16 * 1024 * 1024
PIECES = 8
LOAD_LIMIT = 47 * 1024 * 1024

vmem = pl.BlockSpec(memory_space=pltpu.VMEM)
hbm = pl.BlockSpec(memory_space=pltpu.HBM)


def rows8(ref_value):
    return ref_value.reshape(-1, SUB, ref_value.shape[-1])


def diagonal(width):
    row = lax.broadcasted_iota(jnp.int32, (width, width), 0)
    lane = lax.broadcasted_iota(jnp.int32, (width, width), 1)
    return rows8(row == lane)


def three_terms(value):
    high = value.astype(jnp.bfloat16).astype(jnp.float32)
    middle = (value - high).astype(jnp.bfloat16).astype(jnp.float32)
    return high, middle, (value - high) - middle


def copy_in(source, target, sem):
    return pltpu.make_async_copy(source, target, sem)


def gather_rows(scaled, lookup, picked):
    slots, tiles, width = lookup.shape
    groups = [scaled[n : n + SUB] for n in range(0, scaled.shape[0], SUB)]
    for j in range(slots):
        for start in range(0, tiles, SUB):
            wanted = lookup[j, start : start + SUB, :]
            within = lax.rem(wanted, SUB)
            total = None
            for n, group in enumerate(groups):
                found = jnp.take_along_axis(
                    group, within, axis=0, mode="promise_in_bounds"
                )
                found = jnp.where(wanted // SUB == n, found, 0.0)
                total = found if total is None else total + found
            picked[j, start : start + SUB, :] = total


def forward(jac, picked, rows):
    tiles, slots, width, _ = jac.shape
    eye = diagonal(width)
    for t in range(tiles):
        total = None
        for j in range(slots):
            term = rows8(jac[t, j]) * picked[j, t : t + 1, :][None]
            total = term if total is None else total + term
        total = jnp.sum(total, axis=-1, keepdims=True)
        rows[t : t + 1, :] = jnp.sum(
            jnp.sum(jnp.where(eye, total, 0.0), axis=0), axis=0, keepdims=True
        )


def backward(jac, weighted, picks, spots, back, square):
    tiles, slots, width, _ = jac.shape
    value = weighted[...]
    terms = three_terms(value)
    rest = jnp.zeros((width - 3 * tiles, width), jnp.float32)
    turned = jnp.transpose(jnp.concatenate([*terms, rest], axis=0))
    turned = turned.astype(jnp.bfloat16)
    for t in range(tiles):
        if t % 2 == 0:
            both = jnp.dot(turned, picks[t // 2], preferred_element_type=jnp.float32)
        column = rows8(both[:, t % 2 * width : (t % 2 + 1) * width])
        for j in range(slots):
            block = rows8(jac[t, j])
            if square:
                block = block * block
            back[j * tiles + t : j * tiles + t + 1, :] = jnp.sum(
                jnp.sum(block * column, axis=0), axis=0, keepdims=True
            )
    terms = three_terms(back[...])
    stacked = jnp.concatenate([*terms, jnp.zeros_like(terms[0])], axis=0)
    return jnp.dot(
        spots[...], stacked.astype(jnp.bfloat16), preferred_element_type=jnp.float32
    )


def publish(chunk, out):
    for member in range(out.shape[0]):
        out[member] = chunk


def place_blocks(out, keep, columns, scalars):
    regions, per_dev = out.shape[0], columns.shape[0] // 3
    region = lax.axis_index("region")
    first, middle, last = (
        columns[n * per_dev : (n + 1) * per_dev] for n in range(3)
    )
    keep[...] = jnp.concatenate([columns, scalars], axis=0)
    blank = jnp.concatenate([jnp.zeros_like(first)] * 2 + [scalars], axis=0)
    for away in range(3, regions - 2):
        out[lax.rem(region + away, regions)] = blank
    zero = jnp.zeros_like(first)
    for away, pair in (
        (-2, (first, zero)), (-1, (first, middle)), (1, (middle, last)), (2, (zero, last)),
    ):
        target = lax.rem(region + (away + regions), regions)
        out[target] = jnp.concatenate([*pair, scalars], axis=0)
    out[region] = blank


def load_kernel(jac, held, picks, sems):
    step = jac.shape[0] // PIECES
    pieces = [pl.ds(n * step, step) for n in range(PIECES)]
    copies = [
        copy_in(jac.at[piece], held.at[piece], sems.at[n])
        for n, piece in enumerate(pieces)
    ]
    for copy in copies:
        copy.start()
    tiles, width = jac.shape[0], jac.shape[-1]
    row = lax.broadcasted_iota(jnp.int32, picks.shape[1:], 0)
    half = lax.broadcasted_iota(jnp.int32, picks.shape[1:], 1) // width
    apart = jnp.where(row < 3 * tiles, row % tiles - half, -1)
    for pair in range(picks.shape[0]):
        picks[pair] = jnp.where(apart == 2 * pair, 1.0, 0.0).astype(jnp.bfloat16)
    for copy in copies:
        copy.wait()


def diag_kernel(jac, vectors, picks, *refs):
    ins, (out, weight, spots, lookup, fits, back) = refs[:-6], refs[-6:]
    tiles, slots, width, _ = jac.shape
    blocks = len(ins)
    per_dev = tiles // blocks
    group = lax.axis_index("blk")
    for shift, part in enumerate(ins):
        source = lax.rem(group + (blocks - shift), blocks)
        spot = pl.ds(pl.multiple_of(source * per_dev, per_dev), per_dev)
        weight[spot, :] = part[:per_dev, :]
        fits[spot, :] = part[per_dev:, :]
    lane = lax.broadcasted_iota(jnp.int32, fits.shape, 1)
    chosen = []
    for j in range(slots):
        own = jnp.where(lane == group * slots + j, fits[...], 0.0)
        own = jnp.sum(own, axis=1, keepdims=True)
        chosen.append(jnp.broadcast_to(own, fits.shape))
        lookup[j] = chosen[j].astype(jnp.int32)
    unused = jnp.full((slots * tiles, width), -1.0, jnp.float32)
    names = jnp.transpose(jnp.concatenate(chosen * 3 + [unused], axis=0))
    names = names[: spots.shape[0]].astype(jnp.int32)
    column = lax.broadcasted_iota(jnp.int32, names.shape, 0)
    spots[...] = jnp.where(column == names, 1.0, 0.0).astype(jnp.bfloat16)
    squares = backward(jac, weight, picks, spots, back, True)
    publish(jnp.concatenate([squares, vectors[...]], axis=0), out)


def back_kernel(jac, weight, picks, spots, own, *refs):
    others, (out, keep, weighted, back) = refs[:-4], refs[-4:]
    tiles, slots = jac.shape[:2]
    parts = [own] + list(others)
    even, odd = None, None
    for shift, part in enumerate(parts):
        if shift % 2 == 0:
            even = part[...] if even is None else even + part[...]
        else:
            odd = part[...] if odd is None else odd + part[...]
    total = even if odd is None else even + odd
    rows, sums = total[:tiles], total[tiles:]
    weighted[...] = weight[...] * rows
    delta = jnp.sum(weighted[...] * rows, axis=0, keepdims=True) + sums[1:2]
    scalars = jnp.concatenate([sums[:1], delta, sums[2:]], axis=0)
    columns = backward(jac, weighted, picks, spots, back, False)
    place_blocks(out, keep, columns, scalars)


def send_rows(jac, lookup, resid, scaled, diag, picked, own, out):
    tiles = jac.shape[0]
    gather_rows(scaled, lookup, picked)
    forward(jac, picked, out)
    r, z, d = resid[own], scaled[own], diag[own]
    gamma = jnp.sum(r * z, axis=0, keepdims=True)
    delta = jnp.sum(d * z * z, axis=0, keepdims=True)
    pad = jnp.zeros((SUB - 2, z.shape[1]), jnp.float32)
    out[tiles:, :] = jnp.concatenate([gamma, delta, pad], axis=0)


def gathered(received, region, regions, per_dev):
    blocks = []
    for offset in (-1, 0, 1):
        total = None
        for e in (-1, 0, 1):
            source = lax.rem(region + (offset + e + regions), regions)
            start = (1 - e) * per_dev
            term = received[source, start : start + per_dev, :]
            total = term if total is None else total + term
        blocks.append(total)
    return jnp.concatenate(blocks, axis=0)


def halo(received, region, regions, start, per_dev):
    blocks = []
    for offset in (-1, 0, 1):
        source = lax.rem(region + (offset + regions), regions)
        blocks.append(received[source, start : start + per_dev, :])
    return jnp.concatenate(blocks, axis=0)


def first_kernel(jac, lookup, received, out, diag, precond, resid, picked):
    regions = received.shape[0]
    per_dev = diag.shape[0] // 3
    region = lax.axis_index("region")
    extent = 3 * per_dev
    d = halo(received, region, regions, extent, per_dev)
    r = halo(received, region, regions, extent + per_dev, per_dev)
    m = d + gathered(received, region, regions, per_dev)
    diag[...] = d
    precond[...] = m
    resid[...] = r
    own = slice(per_dev, 2 * per_dev)
    send_rows(jac, lookup, r, r / m, d, picked, own, out)


def collected(received, kept, per_dev):
    regions = received.shape[0]
    region = lax.axis_index("region")
    blocks = []
    for offset in (-1, 0, 1):
        total = None
        for e in (-1, 0, 1):
            away = offset + e
            if away == 0:
                start = (1 - e) * per_dev
                term = kept[start : start + per_dev, :]
            else:
                source = lax.rem(region + (away + regions), regions)
                start = SPOTS[away, offset] * per_dev
                term = received[source, start : start + per_dev, :]
            total = term if total is None else total + term
        blocks.append(total)
    return jnp.concatenate(blocks, axis=0)


def update(received, kept, diag, precond, resid, along, direct, answer, scal):
    regions = received.shape[0]
    per_dev = direct.shape[0]
    r, d, m = resid[...], diag[...], precond[...]
    z = r / m
    image = d * z + collected(received, kept, per_dev)
    region = lax.axis_index("region")
    sums = None
    for member in range(regions):
        term = jnp.where(
            region == member, kept[3 * per_dev :, :], received[member, 2 * per_dev :, :]
        )
        sums = term if sums is None else sums + term
    sums = jnp.sum(sums, axis=1, keepdims=True)
    gamma, delta = sums[:1], sums[1:2]
    before, alpha = scal[0:1, :1], scal[1:2, :1]
    started = alpha != 0.0
    beta = jnp.where(started, gamma / jnp.where(started, before, 1.0), 0.0)
    fall = jnp.where(started, beta * gamma / jnp.where(started, alpha, 1.0), 0.0)
    alpha = gamma / (delta - fall)
    s = image + beta * along[...]
    p = z[per_dev : 2 * per_dev] + beta * direct[...]
    x = answer[...] + alpha * p
    return x, r - alpha * s, s, p, gamma, alpha


def step_kernel(
    jac, lookup, received, kept, diag, precond, resid, along, direct, answer, scal,
    out, resid_o, along_o, direct_o, answer_o, scal_o, picked,
):
    per_dev = direct.shape[0]
    x, r, s, p, gamma, alpha = update(
        received, kept, diag, precond, resid, along, direct, answer, scal
    )
    resid_o[...] = r
    along_o[...] = s
    direct_o[...] = p
    answer_o[...] = x
    scal_o[0:1, :] = jnp.broadcast_to(gamma, (1, scal_o.shape[1]))
    scal_o[1:2, :] = jnp.broadcast_to(alpha, (1, scal_o.shape[1]))
    own = slice(per_dev, 2 * per_dev)
    send_rows(jac, lookup, r, r / precond[...], diag, picked, own, out)


def last_kernel(
    received, kept, diag, precond, resid, along, direct, answer, scal, answer_o,
    resid_o,
):
    per_dev = direct.shape[0]
    x, r, _, _, _, _ = update(
        received, kept, diag, precond, resid, along, direct, answer, scal
    )
    answer_o[...] = x
    resid_o[...] = r[per_dev : 2 * per_dev]


def call(kernel, outs, scratch, specs, name, flops, moved, limit=VMEM_LIMIT):
    outs = [
        shape
        if isinstance(shape, jax.ShapeDtypeStruct)
        else jax.ShapeDtypeStruct(shape, jnp.float32)
        for shape in outs
    ]
    return pl.pallas_call(
        kernel,
        out_shape=outs,
        in_specs=specs,
        out_specs=[vmem] * len(outs),
        scratch_shapes=scratch,
        compiler_params=pltpu.CompilerParams(vmem_limit_bytes=limit),
        cost_estimate=pl.CostEstimate(
            flops=flops, bytes_accessed=moved, transcendentals=0
        ),
        name=name,
    )


def body(jac, pattern, branch_weight, bus_diag, right_side):
    blocks = lax.axis_size("blk")
    regions = lax.axis_size("region")
    per_dev, width = right_side.shape
    tiles, slots = jac.shape[:2]
    extent = 3 * per_dev
    f32 = jnp.float32

    def across_blk(value):
        return [
            lax.ppermute(value, "blk", [(i, (i + k) % blocks) for i in range(blocks)])
            for k in range(1, blocks)
        ]

    def across_region(chunks):
        return lax.all_to_all(chunks, "region", 0, 0, tiled=True)

    flops = 4 * jac.size
    moved = 4 * jac.size
    row_count = tiles + SUB
    picked = pltpu.VMEM((slots, tiles, width), f32)
    back = pltpu.VMEM((tiles * slots, width), f32)
    chunk = (regions, 2 * per_dev + SUB, width)
    kept_shape = (extent + SUB, width)
    halo_shape, own_shape = (extent, width), (per_dev, width)

    spare = width - pattern.shape[1]
    small = [branch_weight, jnp.pad(pattern, ((0, 0), (0, spare))), bus_diag, right_side]
    packed = sum(
        jnp.pad(value, ((n * per_dev, (3 - n) * per_dev), (0, 0))).astype(f32)
        for n, value in enumerate(small)
    )
    packed = lax.optimization_barrier(packed)
    mine, vectors = packed[: 2 * per_dev], packed[2 * per_dev :]
    parts = [mine] + across_blk(mine)
    jac, picks = call(
        load_kernel,
        [
            jac.shape,
            jax.ShapeDtypeStruct((tiles // 2, width, 2 * width), jnp.bfloat16),
        ],
        [pltpu.SemaphoreType.DMA((PIECES,))], [hbm], "load", flops, moved, LOAD_LIMIT,
    )(jac)
    setup, weight, spots, lookup = call(
        diag_kernel,
        [
            (regions, extent + 2 * per_dev, width), (tiles, width),
            jax.ShapeDtypeStruct((extent, 4 * tiles * slots), jnp.bfloat16),
            jax.ShapeDtypeStruct((slots, tiles, width), jnp.int32),
        ],
        [pltpu.VMEM((tiles, width), f32), back],
        [vmem] * (3 + blocks), "diagonal", flops, moved,
    )(jac, vectors, picks, *parts)
    setup = across_region(setup)
    out, diag, precond, resid = call(
        first_kernel, [(row_count, width), halo_shape, halo_shape, halo_shape],
        [picked], [vmem] * 3, "first", flops, moved,
    )(jac, lookup, setup)

    def image_of(out):
        parts = across_blk(out)
        chunks, kept = call(
            back_kernel, [chunk, kept_shape], [pltpu.VMEM((tiles, width), f32), back],
            [vmem] * (5 + len(parts)), "back", flops, moved,
        )(jac, weight, picks, spots, out, *parts)
        return across_region(chunks), kept

    def step(carry):
        received, kept, resid, along, direct, answer, scal = carry
        out, resid, along, direct, answer, scal = call(
            step_kernel,
            [(row_count, width), halo_shape, halo_shape, own_shape, own_shape, (SUB, width)],
            [picked], [vmem] * 11, "step", flops, moved,
        )(jac, lookup, received, kept, diag, precond, resid, along, direct, answer, scal)
        return *image_of(out), resid, along, direct, answer, scal

    carry = (
        *image_of(out), resid, jnp.zeros(halo_shape, f32), jnp.zeros(own_shape, f32),
        jnp.zeros(own_shape, f32), jnp.zeros((SUB, width), f32),
    )
    for _ in range(ITERS - 1):
        carry = step(carry)
    received, kept, resid, along, direct, answer, scal = carry
    answer, resid = call(
        last_kernel, [own_shape, own_shape], [], [vmem] * 9, "last", 1000, 1000
    )(received, kept, diag, precond, resid, along, direct, answer, scal)
    return answer, resid


def solution(mesh):
    both = P(("region", "blk"), None)
    return jax.shard_map(
        body,
        mesh=mesh,
        in_specs=(P("region", "blk", None, None), both, both, both, both),
        out_specs=(both, both),
        check_vma=False,
    )
```

```python
import functools
import jax
import jax.numpy as jnp
from jax import lax
from jax.experimental import pallas as pl
from jax.experimental.pallas import tpu as pltpu
from jax.sharding import PartitionSpec as P

ITERS = 12
SUB = 8
SPOTS = {(2, 1): 0, (1, 0): 0, (1, 1): 1, (-1, -1): 0, (-1, 0): 1, (-2, -1): 1}
VMEM_LIMIT = 16 * 1024 * 1024
PIECES = 8
LOAD_LIMIT = 47 * 1024 * 1024

vmem = pl.BlockSpec(memory_space=pltpu.VMEM)
hbm = pl.BlockSpec(memory_space=pltpu.HBM)


def rows8(ref_value):
    return ref_value.reshape(-1, SUB, ref_value.shape[-1])


def diagonal(width):
    row = lax.broadcasted_iota(jnp.int32, (width, width), 0)
    lane = lax.broadcasted_iota(jnp.int32, (width, width), 1)
    return rows8(row == lane)


def three_terms(value):
    high = value.astype(jnp.bfloat16).astype(jnp.float32)
    middle = (value - high).astype(jnp.bfloat16).astype(jnp.float32)
    return high, middle, (value - high) - middle


def partners(blocks):
    assert blocks & (blocks - 1) == 0
    return sorted(range(1, blocks), key=lambda mask: (mask != blocks // 2, mask))


def copy_in(source, target, sem):
    return pltpu.make_async_copy(source, target, sem)


def gather_rows(scaled, lookup, picked):
    slots, tiles, width = lookup.shape
    groups = [scaled[n : n + SUB] for n in range(0, scaled.shape[0], SUB)]
    for j in range(slots):
        for start in range(0, tiles, SUB):
            wanted = lookup[j, start : start + SUB, :]
            within = lax.rem(wanted, SUB)
            total = None
            for n, group in enumerate(groups):
                found = jnp.take_along_axis(
                    group, within, axis=0, mode="promise_in_bounds"
                )
                found = jnp.where(wanted // SUB == n, found, 0.0)
                total = found if total is None else total + found
            picked[j, start : start + SUB, :] = total


def forward(jac, picked, rows):
    tiles, slots, width, _ = jac.shape
    eye = diagonal(width)
    for t in range(tiles):
        total = None
        for j in range(slots):
            term = rows8(jac[t, j]) * picked[j, t : t + 1, :][None]
            total = term if total is None else total + term
        total = jnp.sum(total, axis=-1, keepdims=True)
        rows[t : t + 1, :] = jnp.sum(
            jnp.sum(jnp.where(eye, total, 0.0), axis=0), axis=0, keepdims=True
        )


def backward(jac, weighted, picks, spots, back, square):
    tiles, slots, width, _ = jac.shape
    value = weighted[...]
    terms = three_terms(value)
    rest = jnp.zeros((width - 3 * tiles, width), jnp.float32)
    turned = jnp.transpose(jnp.concatenate([*terms, rest], axis=0))
    turned = turned.astype(jnp.bfloat16)
    for t in range(tiles):
        if t % 2 == 0:
            both = jnp.dot(turned, picks[t // 2], preferred_element_type=jnp.float32)
        column = rows8(both[:, t % 2 * width : (t % 2 + 1) * width])
        for j in range(slots):
            block = rows8(jac[t, j])
            if square:
                block = block * block
            back[j * tiles + t : j * tiles + t + 1, :] = jnp.sum(
                jnp.sum(block * column, axis=0), axis=0, keepdims=True
            )
    terms = three_terms(back[...])
    stacked = jnp.concatenate([*terms, jnp.zeros_like(terms[0])], axis=0)
    return jnp.dot(
        spots[...], stacked.astype(jnp.bfloat16), preferred_element_type=jnp.float32
    )


def place_blocks(out, keep, columns, scalars):
    regions, per_dev = out.shape[0], columns.shape[0] // 3
    region = lax.axis_index("region")
    first, middle, last = (
        columns[n * per_dev : (n + 1) * per_dev] for n in range(3)
    )
    keep[...] = jnp.concatenate([columns, scalars], axis=0)
    blank = jnp.concatenate([jnp.zeros_like(first)] * 2 + [scalars], axis=0)
    for away in range(3, regions - 2):
        out[lax.rem(region + away, regions)] = blank
    zero = jnp.zeros_like(first)
    for away, pair in (
        (-2, (first, zero)), (-1, (first, middle)), (1, (middle, last)), (2, (zero, last)),
    ):
        target = lax.rem(region + (away + regions), regions)
        out[target] = jnp.concatenate([*pair, scalars], axis=0)
    out[region] = blank


def load_kernel(jac, held, picks, sems):
    step = jac.shape[0] // PIECES
    pieces = [pl.ds(n * step, step) for n in range(PIECES)]
    copies = [
        copy_in(jac.at[piece], held.at[piece], sems.at[n])
        for n, piece in enumerate(pieces)
    ]
    for copy in copies:
        copy.start()
    tiles, width = jac.shape[0], jac.shape[-1]
    row = lax.broadcasted_iota(jnp.int32, picks.shape[1:], 0)
    half = lax.broadcasted_iota(jnp.int32, picks.shape[1:], 1) // width
    apart = jnp.where(row < 3 * tiles, row % tiles - half, -1)
    for pair in range(picks.shape[0]):
        picks[pair] = jnp.where(apart == 2 * pair, 1.0, 0.0).astype(jnp.bfloat16)
    for copy in copies:
        copy.wait()


def diag_kernel(jac, vectors, picks, *refs):
    ins, refs = refs[:-7], refs[-7:]
    out, keep, weight, spots, lookup, fits, back = refs
    tiles, slots, width, _ = jac.shape
    blocks = len(ins)
    per_dev = tiles // blocks
    group = lax.axis_index("blk")
    for mask, part in zip([0] + partners(blocks), ins):
        source = lax.bitwise_xor(group, mask)
        spot = pl.ds(pl.multiple_of(source * per_dev, per_dev), per_dev)
        weight[spot, :] = part[:per_dev, :]
        fits[spot, :] = part[per_dev:, :]
    lane = lax.broadcasted_iota(jnp.int32, fits.shape, 1)
    chosen = []
    for j in range(slots):
        own = jnp.where(lane == group * slots + j, fits[...], 0.0)
        own = jnp.sum(own, axis=1, keepdims=True)
        chosen.append(jnp.broadcast_to(own, fits.shape))
        lookup[j] = chosen[j].astype(jnp.int32)
    unused = jnp.full((slots * tiles, width), -1.0, jnp.float32)
    names = jnp.transpose(jnp.concatenate(chosen * 3 + [unused], axis=0))
    names = names[: spots.shape[0]].astype(jnp.int32)
    column = lax.broadcasted_iota(jnp.int32, names.shape, 0)
    spots[...] = jnp.where(column == names, 1.0, 0.0).astype(jnp.bfloat16)
    squares = backward(jac, weight, picks, spots, back, True)
    place_blocks(out, keep, squares, vectors[...])


def back_kernel(jac, weight, picks, spots, own, *refs):
    others, (out, keep, weighted, back) = refs[:-4], refs[-4:]
    tiles, slots = jac.shape[:2]
    parts = dict(zip([0] + partners(len(others) + 1), [own, *others]))
    total = None
    for mask in range(0, len(parts), 2):
        pair = parts[mask][...] + parts[mask + 1][...]
        total = pair if total is None else total + pair
    rows, sums = total[:tiles], total[tiles:]
    weighted[...] = weight[...] * rows
    delta = jnp.sum(weighted[...] * rows, axis=0, keepdims=True) + sums[1:2]
    scalars = jnp.concatenate([sums[:1], delta, sums[2:]], axis=0)
    columns = backward(jac, weighted, picks, spots, back, False)
    place_blocks(out, keep, columns, scalars)


def send_rows(jac, lookup, resid, scaled, diag, picked, own, out):
    tiles = jac.shape[0]
    gather_rows(scaled, lookup, picked)
    forward(jac, picked, out)
    r, z, d = resid[own], scaled[own], diag[own]
    gamma = jnp.sum(r * z, axis=0, keepdims=True)
    delta = jnp.sum(d * z * z, axis=0, keepdims=True)
    pad = jnp.zeros((SUB - 2, z.shape[1]), jnp.float32)
    out[tiles:, :] = jnp.concatenate([gamma, delta, pad], axis=0)


def collected(received, kept, per_dev):
    regions = received.shape[0]
    region = lax.axis_index("region")
    blocks = []
    for offset in (-1, 0, 1):
        total = None
        for e in (-1, 0, 1):
            away = offset + e
            if away == 0:
                start = (1 - e) * per_dev
                term = kept[start : start + per_dev, :]
            else:
                source = lax.rem(region + (away + regions), regions)
                start = SPOTS[away, offset] * per_dev
                term = received[source, start : start + per_dev, :]
            total = term if total is None else total + term
        blocks.append(total)
    return jnp.concatenate(blocks, axis=0)


def first_kernel(jac, lookup, received, kept, out, diag, precond, resid, picked):
    regions = received.shape[0]
    per_dev = diag.shape[0] // 3
    region = lax.axis_index("region")

    def halo(place):
        blocks = []
        for offset in (-1, 0, 1):
            if offset == 0:
                start = (3 + place) * per_dev
                blocks.append(kept[start : start + per_dev, :])
            else:
                source = lax.rem(region + (offset + regions), regions)
                start = (2 + place) * per_dev
                blocks.append(received[source, start : start + per_dev, :])
        return jnp.concatenate(blocks, axis=0)

    d, r = halo(0), halo(1)
    inverse = 1.0 / (d + collected(received, kept, per_dev))
    diag[...] = d
    precond[...] = inverse
    resid[...] = r
    own = slice(per_dev, 2 * per_dev)
    send_rows(jac, lookup, r, r * inverse, d, picked, own, out)


def update(received, kept, diag, precond, resid, along, direct, answer, scal):
    regions = received.shape[0]
    per_dev = direct.shape[0]
    r, d, inverse = resid[...], diag[...], precond[...]
    z = r * inverse
    image = d * z + collected(received, kept, per_dev)
    region = lax.axis_index("region")
    sums = None
    for member in range(regions):
        term = jnp.where(
            region == member, kept[3 * per_dev :, :], received[member, 2 * per_dev :, :]
        )
        sums = term if sums is None else sums + term
    sums = jnp.sum(sums, axis=1, keepdims=True)
    gamma, delta = sums[:1], sums[1:2]
    beta = gamma * scal[0:1, :1]
    fall = beta * gamma * scal[1:2, :1]
    alpha = gamma / (delta - fall)
    s = image + beta * along[...]
    p = z[per_dev : 2 * per_dev] + beta * direct[...]
    x = answer[...] + alpha * p
    return x, r - alpha * s, s, p, gamma, alpha


def step_kernel(
    jac, lookup, received, kept, diag, precond, resid, along, direct, answer, scal,
    out, resid_o, along_o, direct_o, answer_o, scal_o, picked,
):
    per_dev = direct.shape[0]
    x, r, s, p, gamma, alpha = update(
        received, kept, diag, precond, resid, along, direct, answer, scal
    )
    resid_o[...] = r
    along_o[...] = s
    direct_o[...] = p
    answer_o[...] = x
    scal_o[0:1, :] = jnp.broadcast_to(1.0 / gamma, (1, scal_o.shape[1]))
    scal_o[1:2, :] = jnp.broadcast_to(1.0 / alpha, (1, scal_o.shape[1]))
    own = slice(per_dev, 2 * per_dev)
    send_rows(jac, lookup, r, r * precond[...], diag, picked, own, out)


def last_kernel(
    received, kept, diag, precond, resid, along, direct, answer, scal, answer_o,
    resid_o, values, sems,
):
    per_dev = direct.shape[0]
    x, r, _, _, _, _ = update(
        received, kept, diag, precond, resid, along, direct, answer, scal
    )
    values[0] = x
    values[1] = r[per_dev : 2 * per_dev]
    copies = [
        copy_in(values.at[n], target, sems.at[n])
        for n, target in enumerate((answer_o, resid_o))
    ]
    for copy in copies:
        copy.start()
    for copy in copies:
        copy.wait()


def call(
    kernel, outs, scratch, specs, name, flops, moved, limit=VMEM_LIMIT, target=vmem
):
    outs = [
        shape
        if isinstance(shape, jax.ShapeDtypeStruct)
        else jax.ShapeDtypeStruct(shape, jnp.float32)
        for shape in outs
    ]
    return pl.pallas_call(
        kernel,
        out_shape=outs,
        in_specs=specs,
        out_specs=[target] * len(outs),
        scratch_shapes=scratch,
        compiler_params=pltpu.CompilerParams(vmem_limit_bytes=limit),
        cost_estimate=pl.CostEstimate(
            flops=flops, bytes_accessed=moved, transcendentals=0
        ),
        name=name,
    )


def body(jac, pattern, branch_weight, bus_diag, right_side):
    blocks = lax.axis_size("blk")
    regions = lax.axis_size("region")
    per_dev, width = right_side.shape
    tiles, slots = jac.shape[:2]
    extent = 3 * per_dev
    f32 = jnp.float32

    def across_blk(value):
        return [
            lax.ppermute(value, "blk", [(i, i ^ mask) for i in range(blocks)])
            for mask in partners(blocks)
        ]

    def across_region(chunks):
        return lax.all_to_all(chunks, "region", 0, 0, tiled=True)

    flops = 4 * jac.size
    moved = 4 * jac.size
    row_count = tiles + SUB
    picked = pltpu.VMEM((slots, tiles, width), f32)
    back = pltpu.VMEM((tiles * slots, width), f32)
    chunk = (regions, 2 * per_dev + SUB, width)
    kept_shape = (extent + SUB, width)
    halo_shape, own_shape = (extent, width), (per_dev, width)

    spare = width - pattern.shape[1]
    small = [branch_weight, jnp.pad(pattern, ((0, 0), (0, spare))), bus_diag, right_side]
    packed = sum(
        jnp.pad(value, ((n * per_dev, (3 - n) * per_dev), (0, 0))).astype(f32)
        for n, value in enumerate(small)
    )
    packed = lax.optimization_barrier(packed)
    mine, vectors = packed[: 2 * per_dev], packed[2 * per_dev :]
    parts = [mine] + across_blk(mine)
    jac, picks = call(
        load_kernel,
        [
            jac.shape,
            jax.ShapeDtypeStruct((tiles // 2, width, 2 * width), jnp.bfloat16),
        ],
        [pltpu.SemaphoreType.DMA((PIECES,))], [hbm], "load", flops, moved, LOAD_LIMIT,
    )(jac)
    setup, kept, weight, spots, lookup = call(
        diag_kernel,
        [
            (regions, 4 * per_dev, width), (extent + 2 * per_dev, width),
            (tiles, width),
            jax.ShapeDtypeStruct((extent, 4 * tiles * slots), jnp.bfloat16),
            jax.ShapeDtypeStruct((slots, tiles, width), jnp.int32),
        ],
        [pltpu.VMEM((tiles, width), f32), back],
        [vmem] * (3 + blocks), "diagonal", flops, moved,
    )(jac, vectors, picks, *parts)
    setup = across_region(setup)
    out, diag, precond, resid = call(
        first_kernel, [(row_count, width), halo_shape, halo_shape, halo_shape],
        [picked], [vmem] * 4, "first", flops, moved,
    )(jac, lookup, setup, kept)

    def image_of(out):
        parts = across_blk(out)
        chunks, kept = call(
            back_kernel, [chunk, kept_shape], [pltpu.VMEM((tiles, width), f32), back],
            [vmem] * (5 + len(parts)), "back", flops, moved,
        )(jac, weight, picks, spots, out, *parts)
        return across_region(chunks), kept

    def step(carry):
        received, kept, resid, along, direct, answer, scal = carry
        out, resid, along, direct, answer, scal = call(
            step_kernel,
            [(row_count, width), halo_shape, halo_shape, own_shape, own_shape, (SUB, width)],
            [picked], [vmem] * 11, "step", flops, moved,
        )(jac, lookup, received, kept, diag, precond, resid, along, direct, answer, scal)
        return *image_of(out), resid, along, direct, answer, scal

    carry = (
        *image_of(out), resid, jnp.zeros(halo_shape, f32), jnp.zeros(own_shape, f32),
        jnp.zeros(own_shape, f32), jnp.zeros((SUB, width), f32),
    )
    for _ in range(ITERS - 1):
        carry = step(carry)
    received, kept, resid, along, direct, answer, scal = carry
    answer, resid = call(
        last_kernel, [own_shape, own_shape],
        [pltpu.VMEM((2, *own_shape), f32), pltpu.SemaphoreType.DMA((2,))],
        [vmem] * 9, "last", 1000, 1000, VMEM_LIMIT, hbm,
    )(received, kept, diag, precond, resid, along, direct, answer, scal)
    return answer, resid


def solution(mesh):
    both = P(("region", "blk"), None)
    return jax.shard_map(
        body,
        mesh=mesh,
        in_specs=(P("region", "blk", None, None), both, both, both, both),
        out_specs=(both, both),
        check_vma=False,
    )
```
